32 devices in a mesh: groups: 2 (over y), seq: 4 (over z), heads: 2 (over x), sub: 2 (over core).
Axes of the slice: x: 2, y: 2, z: 4, core: 2. Of those that a mesh axis runs over, the one named last changes fastest.
Arguments:
- queries: bfloat16 [2048, 8192], P(('groups', 'seq', 'sub'), 'heads'), parts along dimension 0, may hold values from -400 to 400
- keys: bfloat16 [2048, 1024], P(('groups', 'seq', 'sub'), 'heads'), parts along dimension 0, may hold values from -6 to 6
- values: bfloat16 [2048, 1024], P(('groups', 'seq', 'sub'), 'heads'), parts along dimension 0, may hold values from -18 to 18
- half_order: int32 [32], P('groups'), parts along dimension 0, may hold values from 0 to 15, as said below
- frame_lengths: int32 [16], P('groups'), parts along dimension 0, may hold values from 1 to 256, 1024 in all
- out_proj: bfloat16 [8192, 4096], P('heads', ('seq', 'sub')), may hold values from -0.09375 to 0.09375
- residual_in: bfloat16 [2048, 4096], P(('groups', 'seq', 'sub'), 'heads'), parts along dimension 0, may hold values from -40 to 40
- norm_gain: float32 [4096], P('heads'), may hold values from 0.5 to 1.5
Outputs:
- attended: bfloat16 [2048, 8192], P(('groups', 'seq', 'sub'), 'heads'), parts along dimension 0
- hidden_state: bfloat16 [2048, 4096], P(('groups', 'seq', 'sub'), 'heads'), parts along dimension 0
- normed: bfloat16 [2048, 4096], P(('groups', 'seq', 'sub'), 'heads'), parts along dimension 0
The draws below stay inside these ranges and needn't reach their ends.
There are 2 independent parts, one for each index of `groups`. The reference program is written for one: setup_inputs(seed, part) draws one part's arguments, and reference() takes and returns one part's arrays. A program takes and returns all parts, laid end to end along the dimension named above; an argument that names none is the same for every part. Nothing has to cross between parts.
Inputs may be any that keep to these rules, and one draw needn't show every extreme that they name: `half_order`: a permutation of 0 to 15.
All inputs are finite; a program needn't handle non-finite values.
Results may differ from the reference program's by a relative error of at most 0.005.
Values may be sent and summed in bfloat16 or wider, within the bound.
A program may use at most 128 MiB of HBM per device.

```python
import math
import jax
import jax.numpy as jnp
import numpy as np
from jax import lax

QUERY_HEAD_COUNT = 64
KEY_VALUE_HEADS = 8
HEAD_WIDTH = 128
OUT_WIDTH = 4096
CLIP_TOKENS = 1024
HALF = 64
HALVES = 16
FRAMES = 8
FRAME_MOST = 256


def order_table(key):
    return jax.random.permutation(jax.random.fold_in(key, 11), HALVES).astype(jnp.int32)


def draw_half_order(key, part):
    return order_table(key)


def draw_keys(key, part):
    filled_rows = jax.random.normal(jax.random.fold_in(key, 17), (CLIP_TOKENS, KEY_VALUE_HEADS * HEAD_WIDTH), jnp.float32)
    return jnp.clip(filled_rows, -6.0, 6.0).astype(jnp.bfloat16)


def draw_queries(key, part):
    filled_rows = 1.5 * jax.random.normal(jax.random.fold_in(key, 31), (CLIP_TOKENS, QUERY_HEAD_COUNT * HEAD_WIDTH), jnp.float32)
    return jnp.clip(filled_rows, -400.0, 400.0).astype(jnp.bfloat16)


def draw_residual_in(key, part):
    column_base = jnp.exp(math.log(4.0) * jnp.arange(OUT_WIDTH, dtype=jnp.float32) / OUT_WIDTH) * 0.5
    column_jitter = jnp.exp(jax.random.uniform(jax.random.fold_in(key, 41), (OUT_WIDTH,), jnp.float32, math.log(0.7), math.log(1.4)))
    entries = jax.random.normal(jax.random.fold_in(key, 43), (CLIP_TOKENS, OUT_WIDTH), jnp.float32)
    row_scale = jnp.exp(jax.random.uniform(jax.random.fold_in(key, 47), (CLIP_TOKENS,), jnp.float32, 0.0, math.log(10.0)))
    filled_rows = entries * (column_base * column_jitter)[None, :] * row_scale[:, None]
    return jnp.clip(filled_rows, -40.0, 40.0).astype(jnp.bfloat16)


def strengthened(values, key, source, target, parts, factor):
    owner, partner = [(jnp.arange(values.shape[dim]) // (values.shape[dim] // parts)).reshape([-1 if axis == dim else 1 for axis in range(values.ndim)]) for dim in (source, target)]
    chosen = jax.random.permutation(key, parts)[partner]
    strong = (owner == chosen) | (owner == (partner + parts // 2) % parts)
    return jnp.where(strong, factor * values, values)


def block_scale(stream_key, shape, split, least, top_value):
    loudness, own = 1.0, jax.random.fold_in(stream_key, 6)
    for dim, parts in split:
        draws = jnp.exp(jax.random.uniform(jax.random.fold_in(own, dim), (parts,), jnp.float32, least / len(split), top_value / len(split)))
        loudness = loudness * jnp.repeat(draws, shape[dim] // parts).reshape([-1 if axis == dim else 1 for axis in range(len(shape))])
    return loudness


def profile(count, total, most, skew):
    loads = [(1 << 20) // math.isqrt(grade ** skew) + 1 for grade in range(2, count + 1)]
    spare, counts = total - most - (count - 1), [1] * (count - 1)
    while spare > 0:
        free = [i for i in range(count - 1) if counts[i] < most]
        whole, budget = sum([loads[i] for i in free]), spare
        for i in free:
            more = min(most - counts[i], max(1, budget * loads[i] // whole), spare)
            counts[i] = counts[i] + more
            spare = spare - more
    return np.array([most] + counts)


def ragged(own_key, count, total, reach, slope):
    if count == 2:
        one = jax.random.randint(own_key, (), max(1, total - reach), min(reach, total - 1) + 1)
        return jnp.stack([one, total - one])
    sizes = jnp.asarray(profile(count, total, reach, slope), jnp.int32)
    couples = (count - 1) // 2
    source_of, taker = sizes[1:1 + 2 * couples:2], sizes[2:2 + 2 * couples:2]
    slack = jnp.minimum(source_of - 1, reach - taker)
    passed = jax.random.randint(jax.random.fold_in(own_key, 1), (couples,), 0, 1 << 20) % (slack + 1)
    sizes = sizes.at[1:1 + 2 * couples:2].set(source_of - passed).at[2:2 + 2 * couples:2].set(taker + passed)
    return sizes[jax.random.permutation(jax.random.fold_in(own_key, 2), count)]


def normal_values(key, shape, scale, limit, pieces=(), held_as=jnp.bfloat16):
    gain = block_scale(key, shape, pieces, -0.22, 0.18) if pieces else 1.0
    array = jax.random.normal(key, shape, jnp.float32) * scale * gain
    return jnp.minimum(jnp.maximum(array, -limit), limit).astype(held_as)


def gaussian_with(own_key, extent, deviation, most, cuts, heavy, held_as=jnp.bfloat16):
    array = deviation * jax.random.normal(own_key, extent, jnp.float32)
    if cuts:
        array = array * block_scale(own_key, extent, cuts, -0.22, 0.18)
    return jnp.clip(strengthened(array, jax.random.fold_in(own_key, 3), *heavy), -most, most).astype(held_as)


def setup_inputs(seed: int = 0, part: int = 0) -> dict:
    arg_keys = jax.random.split(jax.random.key(seed), 9)
    part_keys = jax.random.split(jax.random.fold_in(arg_keys[8], part), 9)
    queries = draw_queries(jax.random.fold_in(jax.random.fold_in(arg_keys[8], part), 71), part)
    keys = draw_keys(jax.random.fold_in(jax.random.fold_in(arg_keys[8], part), 71), part)
    values = normal_values(part_keys[2], (CLIP_TOKENS, KEY_VALUE_HEADS * HEAD_WIDTH), 3.0, 18.0, ((0, 8), (1, 2)))
    half_order = draw_half_order(jax.random.fold_in(jax.random.fold_in(arg_keys[8], part), 71), part)
    frame_lengths = ragged(part_keys[4], FRAMES, CLIP_TOKENS, FRAME_MOST, 2).astype(jnp.int32)
    out_proj = gaussian_with(arg_keys[5], (QUERY_HEAD_COUNT * HEAD_WIDTH, OUT_WIDTH), (QUERY_HEAD_COUNT * HEAD_WIDTH) ** -0.5, 0.09375, ((0, 2), (1, 8)), (0, 1, 8, 2.0))
    residual_in = draw_residual_in(jax.random.fold_in(jax.random.fold_in(arg_keys[8], part), 71), part)
    norm_gain = jnp.clip(1.0 + 0.1 * jax.random.normal(arg_keys[7], (OUT_WIDTH,), jnp.float32), 0.5, 1.5)
    return dict(queries=queries, keys=keys, values=values, half_order=half_order, frame_lengths=frame_lengths, out_proj=out_proj, residual_in=residual_in, norm_gain=norm_gain)


def positions_of(half_order):
    row_ids = jnp.arange(CLIP_TOKENS, dtype=jnp.int32)
    return (half_order[row_ids // HALF] * HALF + row_ids % HALF).astype(jnp.int32)

def frame_limits(position, frame_lengths):
    frame_ends = jnp.cumsum(frame_lengths).astype(jnp.int32)
    frame_starts = frame_ends - frame_lengths
    chosen = jnp.where(frame_starts[None, :] <= position[:, None], frame_lengths[None, :], 0)
    return lax.optimization_barrier(jnp.sum(chosen, axis=1)).astype(jnp.int32)

def reference(queries, keys, values, half_order, frame_lengths, out_proj, residual_in, norm_gain):
    group_width = QUERY_HEAD_COUNT // KEY_VALUE_HEADS
    position = positions_of(half_order)
    frame_end = frame_limits(position, frame_lengths)
    query_head_rows = queries.reshape(CLIP_TOKENS, KEY_VALUE_HEADS, group_width, HEAD_WIDTH)
    key_head_rows = keys.reshape(CLIP_TOKENS, KEY_VALUE_HEADS, HEAD_WIDTH)
    value_head_rows = values.reshape(CLIP_TOKENS, KEY_VALUE_HEADS, HEAD_WIDTH)
    block_rows = min(512, CLIP_TOKENS)
    block_count = CLIP_TOKENS // block_rows

    def single_head(kv_head):
        key_one = key_head_rows[:, kv_head].astype(jnp.float32)
        value_one = value_head_rows[:, kv_head].astype(jnp.float32)
        query_one = query_head_rows[:, kv_head]

        def one_block(block_id):
            query_block = lax.dynamic_slice_in_dim(query_one, block_id * block_rows, block_rows, 0).astype(jnp.float32)
            limit_block = lax.dynamic_slice_in_dim(frame_end, block_id * block_rows, block_rows, 0)
            scores = jnp.einsum('qgd,kd->gqk', query_block, key_one) * HEAD_WIDTH ** (-0.5)
            visible = position[None, :] < limit_block[:, None]
            scores = jnp.where(visible[None], scores, -1e+30)
            row_max = lax.optimization_barrier(jnp.max(scores, axis=-1, keepdims=True))
            weights = jnp.where(visible[None], jnp.exp(scores - row_max), 0.0)
            total = lax.optimization_barrier(jnp.sum(weights, axis=-1))
            rounded = weights.astype(jnp.bfloat16).astype(jnp.float32)
            summed = jnp.einsum('gqk,kd->qgd', rounded, value_one)
            return (summed / jnp.transpose(total)[:, :, None]).astype(jnp.bfloat16)
        blocks = lax.map(one_block, jnp.arange(block_count, dtype=jnp.int32))
        return blocks.reshape(CLIP_TOKENS, group_width, HEAD_WIDTH)
    each_head_rows = lax.map(single_head, jnp.arange(KEY_VALUE_HEADS, dtype=jnp.int32))
    attended = jnp.transpose(each_head_rows, (1, 0, 2, 3)).reshape(CLIP_TOKENS, QUERY_HEAD_COUNT * HEAD_WIDTH)
    projected = jnp.dot(attended, out_proj, preferred_element_type=jnp.float32)
    hidden_state = (residual_in.astype(jnp.float32) + projected).astype(jnp.bfloat16)
    widened = hidden_state.astype(jnp.float32)
    energy = lax.optimization_barrier(jnp.sum(widened * widened, axis=-1)) / OUT_WIDTH
    normed = (widened * lax.rsqrt(energy + 1e-06)[:, None] * norm_gain.astype(jnp.float32)[None, :]).astype(jnp.bfloat16)
    return (attended, hidden_state, normed)
```

```python
import jax
import jax.numpy as jnp
from jax import lax
from jax.sharding import PartitionSpec as P

HEAD_WIDTH = 128
OUT_WIDTH = 4096


def shards(queries, keys, values, half_order, frame_lengths, out_proj, residual_in, norm_gain):
    tok_rows = queries.shape[0]
    kv_local = keys.shape[1] // HEAD_WIDTH
    group_width = queries.shape[1] // keys.shape[1]
    half_rows = tok_rows // 2
    own_index = lax.axis_index("seq") * lax.axis_size("sub") + lax.axis_index("sub")
    table_ids = jnp.arange(half_order.shape[0], dtype=jnp.int32)

    def locate(row_ids):
        matches = (row_ids // half_rows)[:, None] == table_ids[None, :]
        offsets = jnp.sum(jnp.where(matches, half_order[None, :], 0), axis=1)
        return offsets * half_rows + row_ids % half_rows

    query_pos = locate(own_index * tok_rows + jnp.arange(tok_rows, dtype=jnp.int32))
    frame_ends = jnp.cumsum(frame_lengths)
    frame_starts = frame_ends - frame_lengths
    frame_limit = jnp.sum(
        jnp.where(frame_starts[None, :] <= query_pos[:, None], frame_lengths[None, :], 0), axis=1
    )
    query_head_rows = queries.reshape(tok_rows, kv_local, group_width, HEAD_WIDTH)
    score_scale = HEAD_WIDTH ** (-0.5)
    initial = (
        jnp.full((kv_local, group_width, tok_rows), -1e30, jnp.float32),
        jnp.zeros((kv_local, group_width, tok_rows), jnp.float32),
        jnp.zeros((kv_local, group_width, tok_rows, HEAD_WIDTH), jnp.float32),
    )
    key_piece = lax.all_gather(keys, ("seq", "sub"), axis=0, tiled=True)
    value_piece = lax.all_gather(values, ("seq", "sub"), axis=0, tiled=True)
    piece_rows = key_piece.shape[0]
    key_pos = locate(jnp.arange(piece_rows, dtype=jnp.int32))

    def absorb_piece(current):
        running_max, denominator, numerator = current
        key_view = key_piece.reshape(piece_rows, kv_local, HEAD_WIDTH)
        value_view = value_piece.reshape(piece_rows, kv_local, HEAD_WIDTH)
        scores = (
            jnp.einsum(
                "qhgd,khd->hgqk", query_head_rows, key_view, preferred_element_type=jnp.float32
            )
            * score_scale
        )
        visible = key_pos[None, :] < frame_limit[:, None]
        scores = jnp.where(visible, scores, -1e30)
        new_max = jnp.maximum(running_max, jnp.max(scores, axis=-1))
        weights = jnp.where(visible, jnp.exp(scores - new_max[..., None]), 0.0)
        denominator = jnp.sum(weights, axis=-1)
        product = jnp.einsum(
            "hgqk,khd->hgqd",
            weights.astype(jnp.bfloat16),
            value_view,
            preferred_element_type=jnp.float32,
        )
        numerator = product
        return (new_max, denominator, numerator)

    running_max, denominator, numerator = lax.cond(
        jnp.min(key_pos) < jnp.max(frame_limit), absorb_piece, lambda current: current, initial
    )
    result = numerator / denominator[..., None]
    attended = (
        jnp.transpose(result, (2, 0, 1, 3))
        .reshape(tok_rows, kv_local * group_width * HEAD_WIDTH)
        .astype(jnp.bfloat16)
    )
    gathered = lax.all_gather(attended, ("seq", "sub"), axis=0, tiled=True)
    column_terms = jnp.dot(gathered, out_proj, preferred_element_type=jnp.float32)
    head_terms = lax.all_to_all(
        column_terms.astype(jnp.bfloat16), ("seq", "sub"), split_axis=0, concat_axis=1, tiled=True
    )
    projected = lax.psum_scatter(
        head_terms, "heads", scatter_dimension=1, tiled=True
    ).astype(jnp.float32)
    hidden_state = (residual_in.astype(jnp.float32) + projected).astype(jnp.bfloat16)
    widened = hidden_state.astype(jnp.float32)
    energy = lax.psum(jnp.sum(widened * widened, axis=1), "heads") / OUT_WIDTH
    normed = (widened * lax.rsqrt(energy + 1e-06)[:, None] * norm_gain[None, :]).astype(
        jnp.bfloat16
    )
    return (attended, hidden_state, normed)


def solution(mesh):
    in_specs = (
        P(("groups", "seq", "sub"), "heads"),
        P(("groups", "seq", "sub"), "heads"),
        P(("groups", "seq", "sub"), "heads"),
        P("groups"),
        P("groups"),
        P("heads", ("seq", "sub")),
        P(("groups", "seq", "sub"), "heads"),
        P("heads"),
    )
    out_specs = (
        P(("groups", "seq", "sub"), "heads"),
        P(("groups", "seq", "sub"), "heads"),
        P(("groups", "seq", "sub"), "heads"),
    )
    return jax.shard_map(shards, mesh=mesh, in_specs=in_specs, out_specs=out_specs, check_vma=False)
```

```python
import functools
import math

import jax
import jax.numpy as jnp
from jax import lax
from jax.experimental import pallas as pl
from jax.experimental.pallas import tpu as pltpu
from jax.sharding import PartitionSpec as P

HEAD_WIDTH = 128
MESH = pl.DeviceIdType.MESH


def kernel(dims, order_ref, frames_ref, q_ref, kv_ref, proj_hbm, res_ref, gain_ref,
           att_out, hidden_out, normed_out,
           kvbuf, attbuf, proj, bias, acc, pbuf, retbuf, ebuf,
           proj_sem, kv_send, kv_recv, at_send, at_recv, ret_send, ret_recv, en_send, en_recv):
    S, C, H, G = dims
    n = S * C
    blocks = n // H
    rows = q_ref.shape[0]
    width = q_ref.shape[1] // G
    cols = proj.shape[1]
    total = n * rows
    z, c, h = lax.axis_index("seq"), lax.axis_index("sub"), lax.axis_index("heads")
    own = z * C + c
    home = own // blocks
    home_slot = own % blocks

    proj_copy = pltpu.make_async_copy(proj_hbm, proj, proj_sem)
    proj_copy.start()

    barrier = pltpu.get_barrier_semaphore()

    def greet(t, carry):
        other = lax.rem(own * H + h + t, n * H)
        place = other // H
        pl.semaphore_signal(
            barrier, inc=1,
            device_id={"seq": place // C, "sub": place % C, "heads": other % H},
            device_id_type=MESH,
        )
        return carry

    lax.fori_loop(1, n * H, greet, 0)

    half_rows = total // order_ref.shape[0]
    per_device = rows // half_rows
    lane = lax.broadcasted_iota(jnp.int32, (1, total), 1)
    key_pos = jnp.zeros((1, total), jnp.int32)
    for t in range(order_ref.shape[0]):
        inside = (lane >= t * half_rows) & (lane < (t + 1) * half_rows)
        key_pos = jnp.where(inside, lane + (order_ref[t] - t) * half_rows, key_pos)
    line = lax.broadcasted_iota(jnp.int32, (rows, 1), 0)
    row_pos = jnp.zeros((rows, 1), jnp.int32)
    for t in range(per_device):
        inside = (line >= t * half_rows) & (line < (t + 1) * half_rows)
        row_pos = jnp.where(inside, line + (order_ref[own * per_device + t] - t) * half_rows, row_pos)
    limit = jnp.zeros((rows, 1), jnp.int32)
    first = jnp.int32(0)
    for f in range(frames_ref.shape[0]):
        limit = limit + jnp.where(first <= row_pos, frames_ref[f], 0)
        first = first + frames_ref[f]
    bias[...] = jnp.where(key_pos < limit, 0.0, -1e30)
    kvbuf[own] = kv_ref[...]

    pl.semaphore_wait(barrier, n * H - 1)

    def hop(src, buf, send, recv, side, zs, cs, g):
        target = ({"seq": jnp.minimum(z + 1, S - 1)}, {"seq": jnp.maximum(z - 1, 0)}, {"sub": (c + 1) % C})[side]
        index = zs * C + cs
        return pltpu.make_async_remote_copy(
            src_ref=src if src is not None else buf.at[index, g],
            dst_ref=buf.at[index, g],
            send_sem=send.at[side, zs, g],
            recv_sem=recv.at[index, g],
            device_id=target,
            device_id_type=MESH,
        )

    def launch(src, buf, send, recv, g):
        @pl.when(z + 1 < S)
        def _():
            hop(src, buf, send, recv, 0, z, c, g).start()

        @pl.when(z > 0)
        def _():
            hop(src, buf, send, recv, 1, z, c, g).start()

        if C > 1:
            hop(src, buf, send, recv, 2, z, c, g).start()

    def relay(buf, send, recv, d, g):
        @pl.when(z - d >= 0)
        def _():
            hop(None, buf, send, recv, 0, z - d, c, g).wait_recv()

            @pl.when(z + 1 < S)
            def _():
                hop(None, buf, send, recv, 0, z - d, c, g).start()

            if C > 1:
                hop(None, buf, send, recv, 2, z - d, c, g).start()

        @pl.when(z + d < S)
        def _():
            hop(None, buf, send, recv, 1, z + d, c, g).wait_recv()

            @pl.when(z > 0)
            def _():
                hop(None, buf, send, recv, 1, z + d, c, g).start()

            if C > 1:
                hop(None, buf, send, recv, 2, z + d, c, g).start()

    def from_partner(buf, send, recv, zs, g):
        if C > 1:
            hop(None, buf, send, recv, 2, zs, (c + 1) % C, g).wait_recv()

    def drain(src, buf, send, recv, zs, g):
        @pl.when((zs <= z) & (z + 1 < S))
        def _():
            hop(src, buf, send, recv, 0, zs, c, g).wait_send()

        @pl.when((zs >= z) & (z > 0))
        def _():
            hop(src, buf, send, recv, 1, zs, c, g).wait_send()

        if C > 1:
            hop(src, buf, send, recv, 2, zs, c, g).wait_send()

    for g in range(G):
        launch(kv_ref.at[g], kvbuf, kv_send, kv_recv, g)

    def kv_gather(g):
        lax.fori_loop(1, S, lambda d, x: (relay(kvbuf, kv_send, kv_recv, d, g), x)[1], 0)
        lax.fori_loop(0, S, lambda s, x: (from_partner(kvbuf, kv_send, kv_recv, s, g), x)[1], 0)

    factor = HEAD_WIDTH ** (-0.5) * math.log2(math.e)
    heads_each = width // HEAD_WIDTH
    pack = 2 if heads_each % 2 == 0 else 1
    span = pack * HEAD_WIDTH

    def attention(g):
        key = kvbuf[:, g, 0].reshape(total, HEAD_WIDTH)
        value = kvbuf[:, g, 1].reshape(total, HEAD_WIDTH)

        def few_heads(b, carry):
            at = pl.multiple_of(g * width + b * span, span)
            q = q_ref[:, pl.ds(at, span)]
            q = jnp.concatenate(
                [q[:, k * HEAD_WIDTH:(k + 1) * HEAD_WIDTH] for k in range(pack)], axis=0
            )
            s = lax.dot_general(q, key, (((1,), (1,)), ((), ())), preferred_element_type=jnp.float32)
            s = (s.reshape(pack, rows, total) + bias[...][None]).reshape(pack * rows, total)
            top = jnp.max(s, axis=-1, keepdims=True)
            w = jnp.exp2((s - top) * factor)
            amount = jnp.sum(w, axis=-1, keepdims=True)
            o = jnp.dot(w.astype(jnp.bfloat16), value, preferred_element_type=jnp.float32)
            o = (o / amount).astype(jnp.bfloat16)
            o = jnp.concatenate([o[k * rows:(k + 1) * rows] for k in range(pack)], axis=1)
            att_out[:, pl.ds(at, span)] = o
            attbuf[own, g, :, pl.ds(pl.multiple_of(b * span, span), span)] = o
            return carry

        lax.fori_loop(0, heads_each // pack, few_heads, 0)

    def result_copy(index):
        return pltpu.make_async_remote_copy(
            src_ref=pbuf.at[index],
            dst_ref=retbuf.at[h, home_slot],
            send_sem=ret_send.at[index],
            recv_sem=ret_recv.at[h, home_slot],
            device_id={"seq": index // C, "sub": index % C, "heads": home},
            device_id_type=MESH,
        )

    def multiply(zb, g, last):
        a = attbuf[pl.ds(zb * C, C), g].reshape(C * rows, width)
        w = proj[pl.ds(pl.multiple_of(g * width, width), width), :]
        at = pl.ds(pl.multiple_of(zb * C * rows, C * rows), C * rows)
        summed = acc[at, :] + jnp.dot(a, w, preferred_element_type=jnp.float32)
        if not last:
            acc[at, :] = summed
            return
        summed = summed.astype(jnp.bfloat16)
        for k in range(C):
            index = zb * C + k
            pbuf[index] = summed[k * rows:(k + 1) * rows]
            here = (index == own) & (home == h)

            @pl.when(here)
            def _():
                retbuf[h, home_slot] = summed[k * rows:(k + 1) * rows]

            @pl.when(jnp.logical_not(here))
            def _():
                result_copy(index).start()

    def process(g, last):
        from_partner(attbuf, at_send, at_recv, z, g)
        multiply(z, g, last)

        def step(d, carry):
            relay(attbuf, at_send, at_recv, d, g)

            @pl.when(z - d >= 0)
            def _():
                from_partner(attbuf, at_send, at_recv, z - d, g)
                multiply(z - d, g, last)

            @pl.when(z + d < S)
            def _():
                from_partner(attbuf, at_send, at_recv, z + d, g)
                multiply(z + d, g, last)

            return carry

        lax.fori_loop(1, S, step, 0)

    acc[...] = jnp.zeros_like(acc)
    lax.fori_loop(0, G, lambda g, x: (kv_gather(g), x)[1], 0)

    def head_step(g, carry):
        attention(g)
        launch(None, attbuf, at_send, at_recv, g)

        @pl.when(g == 0)
        def _():
            proj_copy.wait()

        @pl.when(g > 0)
        def _():
            process(g - 1, False)

        return carry

    lax.fori_loop(0, G, head_step, 0)
    process(G - 1, True)

    squares = jnp.zeros((rows, 1), jnp.float32)
    for b in range(blocks):
        where = slice(b * cols, (b + 1) * cols)
        value = res_ref[:, where].astype(jnp.float32)
        for k in range(H):
            @pl.when(jnp.logical_not((home == h) & (home_slot == b) & (k == h)))
            def _():
                pltpu.make_async_remote_copy(
                    src_ref=pbuf.at[0], dst_ref=retbuf.at[k, b],
                    send_sem=ret_send.at[0], recv_sem=ret_recv.at[k, b],
                    device_id={"heads": home}, device_id_type=MESH,
                ).wait_recv()
            value = value + retbuf[k, b].astype(jnp.float32)
        hidden = value.astype(jnp.bfloat16)
        hidden_out[:, where] = hidden
        wide = hidden.astype(jnp.float32)
        squares = squares + jnp.sum(wide * wide, axis=-1, keepdims=True)

    ebuf[h] = jnp.broadcast_to(squares, (rows, 128))

    def share(k, side):
        other = (h + k) % H if side == 0 else (h + H - k) % H
        return pltpu.make_async_remote_copy(
            src_ref=ebuf.at[h], dst_ref=ebuf.at[h if side == 0 else other],
            send_sem=en_send.at[k], recv_sem=en_recv.at[h if side == 0 else other],
            device_id={"heads": (h + k) % H}, device_id_type=MESH,
        )

    for k in range(1, H):
        share(k, 0).start()
    for k in range(1, H):
        share(k, 1).wait_recv()
    energy = ebuf[0]
    for k in range(1, H):
        energy = energy + ebuf[k]
    inverse = lax.rsqrt(energy[:, 0:1] / (H * res_ref.shape[1]) + 1e-06)
    for b in range(blocks):
        where = slice(b * cols, (b + 1) * cols)
        normed_out[:, where] = (
            hidden_out[:, where].astype(jnp.float32) * inverse * gain_ref[:, where]
        ).astype(jnp.bfloat16)

    for k in range(1, H):
        share(k, 0).wait_send()

    def finish(i, carry):
        zs, g = i // G, i % G
        drain(kv_ref.at[g], kvbuf, kv_send, kv_recv, zs, g)
        drain(None, attbuf, at_send, at_recv, zs, g)
        return carry

    lax.fori_loop(0, S * G, finish, 0)

    def finish_results(index, carry):
        @pl.when(jnp.logical_not((index == own) & (home == h)))
        def _():
            result_copy(index).wait_send()
        return carry

    lax.fori_loop(0, n, finish_results, 0)


def shards(dims, queries, keys, values, half_order, frame_lengths, out_proj, residual_in, norm_gain):
    S, C, H = dims
    n = S * C
    rows = queries.shape[0]
    G = keys.shape[1] // HEAD_WIDTH
    width = queries.shape[1] // G
    cols = out_proj.shape[1]
    kv = jnp.stack(
        [jnp.transpose(a.reshape(rows, G, HEAD_WIDTH), (1, 0, 2)) for a in (keys, values)], axis=1
    )
    vmem = pl.BlockSpec(memory_space=pltpu.VMEM)
    smem = pl.BlockSpec(memory_space=pltpu.SMEM)
    dma = pltpu.SemaphoreType.DMA
    bf16, f32 = jnp.bfloat16, jnp.float32
    return pl.pallas_call(
        functools.partial(kernel, (S, C, H, G)),
        out_shape=(
            jax.ShapeDtypeStruct(queries.shape, bf16),
            jax.ShapeDtypeStruct(residual_in.shape, bf16),
            jax.ShapeDtypeStruct(residual_in.shape, bf16),
        ),
        in_specs=[smem, smem, vmem, vmem, pl.BlockSpec(memory_space=pl.ANY), vmem, vmem],
        out_specs=(vmem, vmem, vmem),
        scratch_shapes=[
            pltpu.VMEM((n, G, 2, rows, HEAD_WIDTH), bf16),
            pltpu.VMEM((n, G, rows, width), bf16),
            pltpu.VMEM(out_proj.shape, bf16),
            pltpu.VMEM((rows, n * rows), f32),
            pltpu.VMEM((n * rows, cols), f32),
            pltpu.VMEM((n, rows, cols), bf16),
            pltpu.VMEM((H, n // H, rows, cols), bf16),
            pltpu.VMEM((H, rows, 128), f32),
            dma(()),
            dma((3, S, G)),
            dma((n, G)),
            dma((3, S, G)),
            dma((n, G)),
            dma((n,)),
            dma((H, n // H)),
            dma((H,)),
            dma((H,)),
        ],
        compiler_params=pltpu.CompilerParams(
            collective_id=0, has_side_effects=True, vmem_limit_bytes=60 * 1024 * 1024
        ),
    )(half_order, frame_lengths, queries, kv, out_proj, residual_in, norm_gain[None, :])


def solution(mesh):
    dims = (mesh.shape["seq"], mesh.shape["sub"], mesh.shape["heads"])
    token = P(("groups", "seq", "sub"), "heads")
    in_specs = (
        token, token, token, P("groups"), P("groups"),
        P("heads", ("seq", "sub")), token, P("heads"),
    )
    return jax.shard_map(
        functools.partial(shards, dims), mesh=mesh, in_specs=in_specs,
        out_specs=(token, token, token), check_vma=False,
    )
```

```python
import functools
import math

import jax
import jax.numpy as jnp
from jax import lax
from jax.experimental import pallas as pl
from jax.experimental.pallas import tpu as pltpu
from jax.sharding import PartitionSpec as P

HEAD_WIDTH = 128
MESH = pl.DeviceIdType.MESH


def kernel(dims, order_ref, frames_ref, q_ref, keys_ref, values_ref, proj_hbm, res_ref, gain_ref,
           att_out, hidden_out, normed_out,
           kvbuf, attbuf, proj, bias, pbuf, retbuf, ebuf,
           proj_sem, kv_send, kv_recv, at_send, at_recv, ret_send, ret_recv, en_send, en_recv):
    S, C, H, G = dims
    n = S * C
    blocks = n // H
    rows = q_ref.shape[0]
    width = q_ref.shape[1] // G
    cols = proj.shape[1]
    total = n * rows
    z, c, h = lax.axis_index("seq"), lax.axis_index("sub"), lax.axis_index("heads")
    own = z * C + c
    home = own // blocks
    home_slot = own % blocks

    proj_copy = pltpu.make_async_copy(proj_hbm, proj, proj_sem)
    proj_copy.start()

    barrier = pltpu.get_barrier_semaphore()

    def greet(t, carry):
        other = lax.rem(own * H + h + t, n * H)
        place = other // H
        pl.semaphore_signal(
            barrier, inc=1,
            device_id={"seq": place // C, "sub": place % C, "heads": other % H},
            device_id_type=MESH,
        )
        return carry

    lax.fori_loop(1, n * H, greet, 0)

    half_rows = total // order_ref.shape[0]
    per_device = rows // half_rows
    lane = lax.broadcasted_iota(jnp.int32, (1, total), 1)
    key_pos = jnp.zeros((1, total), jnp.int32)
    for t in range(order_ref.shape[0]):
        inside = (lane >= t * half_rows) & (lane < (t + 1) * half_rows)
        key_pos = jnp.where(inside, lane + (order_ref[t] - t) * half_rows, key_pos)
    line = lax.broadcasted_iota(jnp.int32, (rows, 1), 0)
    row_pos = jnp.zeros((rows, 1), jnp.int32)
    for t in range(per_device):
        inside = (line >= t * half_rows) & (line < (t + 1) * half_rows)
        row_pos = jnp.where(inside, line + (order_ref[own * per_device + t] - t) * half_rows, row_pos)
    limit = jnp.zeros((rows, 1), jnp.int32)
    first = jnp.int32(0)
    for f in range(frames_ref.shape[0]):
        limit = limit + jnp.where(first <= row_pos, frames_ref[f], 0)
        first = first + frames_ref[f]
    bias[...] = jnp.where(key_pos < limit, 0.0, -1e30)
    for g in range(G):
        part = slice(g * HEAD_WIDTH, (g + 1) * HEAD_WIDTH)
        kvbuf[own, g, 0] = keys_ref[:, part]
        kvbuf[own, g, 1] = values_ref[:, part]

    pl.semaphore_wait(barrier, n * H - 1)

    def hop(buf, send, recv, side, zs, cs, g):
        target = ({"seq": jnp.minimum(z + 1, S - 1)}, {"seq": jnp.maximum(z - 1, 0)}, {"sub": (c + 1) % C})[side]
        index = zs * C + cs
        return pltpu.make_async_remote_copy(
            src_ref=buf.at[index, g],
            dst_ref=buf.at[index, g],
            send_sem=send.at[side, zs, g],
            recv_sem=recv.at[index, g],
            device_id=target,
            device_id_type=MESH,
        )

    def launch(buf, send, recv, g):
        @pl.when(z + 1 < S)
        def _():
            hop(buf, send, recv, 0, z, c, g).start()

        @pl.when(z > 0)
        def _():
            hop(buf, send, recv, 1, z, c, g).start()

        if C > 1:
            hop(buf, send, recv, 2, z, c, g).start()

    def relay(buf, send, recv, d, g):
        @pl.when(z - d >= 0)
        def _():
            hop(buf, send, recv, 0, z - d, c, g).wait_recv()

            @pl.when(z + 1 < S)
            def _():
                hop(buf, send, recv, 0, z - d, c, g).start()

            if C > 1:
                hop(buf, send, recv, 2, z - d, c, g).start()

        @pl.when(z + d < S)
        def _():
            hop(buf, send, recv, 1, z + d, c, g).wait_recv()

            @pl.when(z > 0)
            def _():
                hop(buf, send, recv, 1, z + d, c, g).start()

            if C > 1:
                hop(buf, send, recv, 2, z + d, c, g).start()

    def from_partner(buf, send, recv, zs, g):
        if C > 1:
            hop(buf, send, recv, 2, zs, (c + 1) % C, g).wait_recv()

    def drain(buf, send, recv, zs, g):
        @pl.when((zs <= z) & (z + 1 < S))
        def _():
            hop(buf, send, recv, 0, zs, c, g).wait_send()

        @pl.when((zs >= z) & (z > 0))
        def _():
            hop(buf, send, recv, 1, zs, c, g).wait_send()

        if C > 1:
            hop(buf, send, recv, 2, zs, c, g).wait_send()

    def kv_relay(g):
        @pl.when(g + 1 < G)
        def _():
            launch(kvbuf, kv_send, kv_recv, g + 1)

        lax.fori_loop(1, S, lambda d, x: (relay(kvbuf, kv_send, kv_recv, d, g), x)[1], 0)

    def kv_partner(g):
        lax.fori_loop(0, S, lambda s, x: (from_partner(kvbuf, kv_send, kv_recv, s, g), x)[1], 0)

    factor = HEAD_WIDTH ** (-0.5) * math.log2(math.e)
    heads_each = width // HEAD_WIDTH
    pack = 2 if heads_each % 2 == 0 else 1
    span = pack * HEAD_WIDTH

    def attention(g):
        kv_partner(g)
        key = kvbuf[:, g, 0].reshape(total, HEAD_WIDTH)
        value = kvbuf[:, g, 1].reshape(total, HEAD_WIDTH)

        def few_heads(b, carry):
            at = pl.multiple_of(g * width + b * span, span)
            q = q_ref[:, pl.ds(at, span)]
            q = jnp.concatenate(
                [q[:, k * HEAD_WIDTH:(k + 1) * HEAD_WIDTH] for k in range(pack)], axis=0
            )
            s = lax.dot_general(q, key, (((1,), (1,)), ((), ())), preferred_element_type=jnp.float32)
            s = (s.reshape(pack, rows, total) + bias[...][None]).reshape(pack * rows, total)
            top = jnp.max(s, axis=-1, keepdims=True)
            w = jnp.exp2((s - top) * factor)
            amount = jnp.sum(w, axis=-1, keepdims=True)
            o = jnp.dot(w.astype(jnp.bfloat16), value, preferred_element_type=jnp.float32)
            o = (o / amount).astype(jnp.bfloat16)
            o = jnp.concatenate([o[k * rows:(k + 1) * rows] for k in range(pack)], axis=1)
            att_out[:, pl.ds(at, span)] = o
            attbuf[own, g, :, pl.ds(pl.multiple_of(b * span, span), span)] = o

            @pl.when((g == 0) & (b + 1 < G))
            def _():
                kv_relay(jnp.minimum(b + 1, G - 1))

            return carry

        lax.fori_loop(0, heads_each // pack, few_heads, 0)

        @pl.when(g == 0)
        def _():
            lax.fori_loop(min(heads_each // pack + 1, G), G, lambda k, x: (kv_relay(k), x)[1], 0)

    def result_copy(index):
        return pltpu.make_async_remote_copy(
            src_ref=pbuf.at[index],
            dst_ref=retbuf.at[h, home_slot],
            send_sem=ret_send.at[index],
            recv_sem=ret_recv.at[h, home_slot],
            device_id={"seq": index // C, "sub": index % C, "heads": home},
            device_id_type=MESH,
        )

    def multiply(zb):
        summed = jnp.zeros((C * rows, cols), jnp.float32)
        for g in range(G):
            from_partner(attbuf, at_send, at_recv, zb, g)
            summed = summed + jnp.dot(
                attbuf[pl.ds(zb * C, C), g].reshape(C * rows, width),
                proj[g * width:(g + 1) * width, :],
                preferred_element_type=jnp.float32,
            )
        summed = summed.astype(jnp.bfloat16)
        for k in range(C):
            index = zb * C + k
            pbuf[index] = summed[k * rows:(k + 1) * rows]
            here = (index == own) & (home == h)

            @pl.when(here)
            def _():
                retbuf[h, home_slot] = summed[k * rows:(k + 1) * rows]

            @pl.when(jnp.logical_not(here))
            def _():
                result_copy(index).start()

    launch(kvbuf, kv_send, kv_recv, 0)
    kv_relay(jnp.int32(0))

    def head_step(g, carry):
        attention(g)
        launch(attbuf, at_send, at_recv, g)
        return carry

    lax.fori_loop(0, G, head_step, 0)
    proj_copy.wait()
    multiply(z)

    def step(d, carry):
        lax.fori_loop(0, G, lambda g, x: (relay(attbuf, at_send, at_recv, d, g), x)[1], 0)

        @pl.when(z - d >= 0)
        def _():
            multiply(z - d)

        @pl.when(z + d < S)
        def _():
            multiply(z + d)

        return carry

    lax.fori_loop(1, S, step, 0)

    squares = jnp.zeros((rows, 1), jnp.float32)
    for b in range(blocks):
        where = slice(b * cols, (b + 1) * cols)
        value = res_ref[:, where].astype(jnp.float32)
        for k in range(H):
            @pl.when(jnp.logical_not((home == h) & (home_slot == b) & (k == h)))
            def _():
                pltpu.make_async_remote_copy(
                    src_ref=pbuf.at[0], dst_ref=retbuf.at[k, b],
                    send_sem=ret_send.at[0], recv_sem=ret_recv.at[k, b],
                    device_id={"heads": home}, device_id_type=MESH,
                ).wait_recv()
            value = value + retbuf[k, b].astype(jnp.float32)
        hidden = value.astype(jnp.bfloat16)
        hidden_out[:, where] = hidden
        wide = hidden.astype(jnp.float32)
        squares = squares + jnp.sum(wide * wide, axis=-1, keepdims=True)

    ebuf[h] = jnp.broadcast_to(squares, (rows, 128))

    def share(k, side):
        other = (h + k) % H if side == 0 else (h + H - k) % H
        return pltpu.make_async_remote_copy(
            src_ref=ebuf.at[h], dst_ref=ebuf.at[h if side == 0 else other],
            send_sem=en_send.at[k], recv_sem=en_recv.at[h if side == 0 else other],
            device_id={"heads": (h + k) % H}, device_id_type=MESH,
        )

    for k in range(1, H):
        share(k, 0).start()
    for k in range(1, H):
        share(k, 1).wait_recv()
    energy = ebuf[0]
    for k in range(1, H):
        energy = energy + ebuf[k]
    inverse = lax.rsqrt(energy[:, 0:1] / (H * res_ref.shape[1]) + 1e-06)
    for b in range(blocks):
        where = slice(b * cols, (b + 1) * cols)
        normed_out[:, where] = (
            hidden_out[:, where].astype(jnp.float32) * inverse * gain_ref[:, where]
        ).astype(jnp.bfloat16)

    for k in range(1, H):
        share(k, 0).wait_send()

    def finish(i, carry):
        zs, g = i // G, i % G
        drain(kvbuf, kv_send, kv_recv, zs, g)
        drain(attbuf, at_send, at_recv, zs, g)
        return carry

    lax.fori_loop(0, S * G, finish, 0)

    def finish_results(index, carry):
        @pl.when(jnp.logical_not((index == own) & (home == h)))
        def _():
            result_copy(index).wait_send()
        return carry

    lax.fori_loop(0, n, finish_results, 0)


def shards(dims, queries, keys, values, half_order, frame_lengths, out_proj, residual_in, norm_gain):
    S, C, H = dims
    n = S * C
    rows = queries.shape[0]
    G = keys.shape[1] // HEAD_WIDTH
    width = queries.shape[1] // G
    cols = out_proj.shape[1]
    vmem = pl.BlockSpec(memory_space=pltpu.VMEM)
    smem = pl.BlockSpec(memory_space=pltpu.SMEM)
    dma = pltpu.SemaphoreType.DMA
    bf16, f32 = jnp.bfloat16, jnp.float32
    return pl.pallas_call(
        functools.partial(kernel, (S, C, H, G)),
        out_shape=(
            jax.ShapeDtypeStruct(queries.shape, bf16),
            jax.ShapeDtypeStruct(residual_in.shape, bf16),
            jax.ShapeDtypeStruct(residual_in.shape, bf16),
        ),
        in_specs=[smem, smem, vmem, vmem, vmem, pl.BlockSpec(memory_space=pl.ANY), vmem, vmem],
        out_specs=(vmem, vmem, vmem),
        scratch_shapes=[
            pltpu.VMEM((n, G, 2, rows, HEAD_WIDTH), bf16),
            pltpu.VMEM((n, G, rows, width), bf16),
            pltpu.VMEM(out_proj.shape, bf16),
            pltpu.VMEM((rows, n * rows), f32),
            pltpu.VMEM((n, rows, cols), bf16),
            pltpu.VMEM((H, n // H, rows, cols), bf16),
            pltpu.VMEM((H, rows, 128), f32),
            dma(()),
            dma((3, S, G)),
            dma((n, G)),
            dma((3, S, G)),
            dma((n, G)),
            dma((n,)),
            dma((H, n // H)),
            dma((H,)),
            dma((H,)),
        ],
        compiler_params=pltpu.CompilerParams(
            collective_id=0, has_side_effects=True, vmem_limit_bytes=40 * 1024 * 1024
        ),
    )(half_order, frame_lengths, queries, keys, values, out_proj, residual_in, norm_gain[None, :])


def solution(mesh):
    dims = (mesh.shape["seq"], mesh.shape["sub"], mesh.shape["heads"])
    token = P(("groups", "seq", "sub"), "heads")
    in_specs = (
        token, token, token, P("groups"), P("groups"),
        P("heads", ("seq", "sub")), token, P("heads"),
    )
    return jax.shard_map(
        functools.partial(shards, dims), mesh=mesh, in_specs=in_specs,
        out_specs=(token, token, token), check_vma=False,
    )
```

```python
import functools
import math

import jax
import jax.numpy as jnp
from jax import lax
from jax.experimental import pallas as pl
from jax.experimental.pallas import tpu as pltpu
from jax.sharding import PartitionSpec as P

HEAD_WIDTH = 128
MESH = pl.DeviceIdType.MESH


def kernel(dims, order_ref, frames_ref, q_hbm, keys_ref, values_ref, proj_hbm, res_hbm, gain_ref,
           att_out, hidden_out, normed_out,
           kvbuf, attbuf, proj, q_ref, res_ref, bias, pbuf, retbuf, ebuf,
           in_sem, kv_send, kv_recv, at_send, at_recv, ret_send, ret_recv, en_send, en_recv):
    S, C, H, G = dims
    n = S * C
    blocks = n // H
    rows = q_ref.shape[0]
    width = q_ref.shape[1] // G
    cols = proj.shape[1]
    total = n * rows
    z, c, h = lax.axis_index("seq"), lax.axis_index("sub"), lax.axis_index("heads")
    own = z * C + c
    home = own // blocks
    home_slot = own % blocks

    q_copy = pltpu.make_async_copy(q_hbm, q_ref, in_sem.at[0])
    q_copy.start()
    proj_copy = pltpu.make_async_copy(proj_hbm, proj, in_sem.at[1])
    proj_copy.start()
    res_copy = pltpu.make_async_copy(res_hbm, res_ref, in_sem.at[2])
    res_copy.start()

    barrier = pltpu.get_barrier_semaphore()

    def greet(t, carry):
        other = lax.rem(own * H + h + t, n * H)
        place = other // H
        pl.semaphore_signal(
            barrier, inc=1,
            device_id={"seq": place // C, "sub": place % C, "heads": other % H},
            device_id_type=MESH,
        )
        return carry

    lax.fori_loop(1, n * H, greet, 0)

    half_rows = total // order_ref.shape[0]
    per_device = rows // half_rows
    lane = lax.broadcasted_iota(jnp.int32, (1, total), 1)
    key_pos = jnp.zeros((1, total), jnp.int32)
    for t in range(order_ref.shape[0]):
        inside = (lane >= t * half_rows) & (lane < (t + 1) * half_rows)
        key_pos = jnp.where(inside, lane + (order_ref[t] - t) * half_rows, key_pos)
    line = lax.broadcasted_iota(jnp.int32, (rows, 1), 0)
    row_pos = jnp.zeros((rows, 1), jnp.int32)
    for t in range(per_device):
        inside = (line >= t * half_rows) & (line < (t + 1) * half_rows)
        row_pos = jnp.where(inside, line + (order_ref[own * per_device + t] - t) * half_rows, row_pos)
    limit = jnp.zeros((rows, 1), jnp.int32)
    first = jnp.int32(0)
    for f in range(frames_ref.shape[0]):
        limit = limit + jnp.where(first <= row_pos, frames_ref[f], 0)
        first = first + frames_ref[f]
    bias[...] = jnp.where(key_pos < limit, 0.0, -1e30)
    for g in range(G):
        part = slice(g * HEAD_WIDTH, (g + 1) * HEAD_WIDTH)
        kvbuf[own, g, 0] = keys_ref[:, part]
        kvbuf[own, g, 1] = values_ref[:, part]

    pl.semaphore_wait(barrier, n * H - 1)

    def hop(buf, send, recv, side, zs, cs, g):
        target = ({"seq": jnp.minimum(z + 1, S - 1)}, {"seq": jnp.maximum(z - 1, 0)}, {"sub": (c + 1) % C})[side]
        index = zs * C + cs
        return pltpu.make_async_remote_copy(
            src_ref=buf.at[index, g],
            dst_ref=buf.at[index, g],
            send_sem=send.at[side, zs, g],
            recv_sem=recv.at[index, g],
            device_id=target,
            device_id_type=MESH,
        )

    def launch(buf, send, recv, g):
        @pl.when(z + 1 < S)
        def _():
            hop(buf, send, recv, 0, z, c, g).start()

        @pl.when(z > 0)
        def _():
            hop(buf, send, recv, 1, z, c, g).start()

        if C > 1:
            hop(buf, send, recv, 2, z, c, g).start()

    def relay(buf, send, recv, d, g):
        @pl.when(z - d >= 0)
        def _():
            hop(buf, send, recv, 0, z - d, c, g).wait_recv()

            @pl.when(z + 1 < S)
            def _():
                hop(buf, send, recv, 0, z - d, c, g).start()

            if C > 1:
                hop(buf, send, recv, 2, z - d, c, g).start()

        @pl.when(z + d < S)
        def _():
            hop(buf, send, recv, 1, z + d, c, g).wait_recv()

            @pl.when(z > 0)
            def _():
                hop(buf, send, recv, 1, z + d, c, g).start()

            if C > 1:
                hop(buf, send, recv, 2, z + d, c, g).start()

    def from_partner(buf, send, recv, zs, g):
        if C > 1:
            hop(buf, send, recv, 2, zs, (c + 1) % C, g).wait_recv()

    def drain(buf, send, recv, zs, g):
        @pl.when((zs <= z) & (z + 1 < S))
        def _():
            hop(buf, send, recv, 0, zs, c, g).wait_send()

        @pl.when((zs >= z) & (z > 0))
        def _():
            hop(buf, send, recv, 1, zs, c, g).wait_send()

        if C > 1:
            hop(buf, send, recv, 2, zs, c, g).wait_send()

    def kv_relay(g):
        @pl.when(g + 1 < G)
        def _():
            launch(kvbuf, kv_send, kv_recv, g + 1)

        lax.fori_loop(1, S, lambda d, x: (relay(kvbuf, kv_send, kv_recv, d, g), x)[1], 0)

    def kv_partner(g):
        lax.fori_loop(0, S, lambda s, x: (from_partner(kvbuf, kv_send, kv_recv, s, g), x)[1], 0)

    factor = HEAD_WIDTH ** (-0.5) * math.log2(math.e)
    heads_each = width // HEAD_WIDTH
    pack = 2 if heads_each % 2 == 0 else 1
    span = pack * HEAD_WIDTH

    def attention(g):
        kv_partner(g)
        key = kvbuf[:, g, 0].reshape(total, HEAD_WIDTH)
        value = kvbuf[:, g, 1].reshape(total, HEAD_WIDTH)

        def few_heads(b, carry):
            at = pl.multiple_of(g * width + b * span, span)
            q = q_ref[:, pl.ds(at, span)]
            q = jnp.concatenate(
                [q[:, k * HEAD_WIDTH:(k + 1) * HEAD_WIDTH] for k in range(pack)], axis=0
            )
            s = lax.dot_general(q, key, (((1,), (1,)), ((), ())), preferred_element_type=jnp.float32)
            s = (s.reshape(pack, rows, total) + bias[...][None]).reshape(pack * rows, total)
            top = jnp.max(s, axis=-1, keepdims=True)
            w = jnp.exp2((s - top) * factor)
            amount = jnp.sum(w, axis=-1, keepdims=True)
            o = jnp.dot(w.astype(jnp.bfloat16), value, preferred_element_type=jnp.float32)
            o = (o / amount).astype(jnp.bfloat16)
            o = jnp.concatenate([o[k * rows:(k + 1) * rows] for k in range(pack)], axis=1)
            att_out[:, pl.ds(at, span)] = o
            attbuf[own, g, :, pl.ds(pl.multiple_of(b * span, span), span)] = o

            @pl.when((g == 0) & (b + 1 < G))
            def _():
                kv_relay(jnp.minimum(b + 1, G - 1))

            return carry

        lax.fori_loop(0, heads_each // pack, few_heads, 0)

        @pl.when(g == 0)
        def _():
            lax.fori_loop(min(heads_each // pack + 1, G), G, lambda k, x: (kv_relay(k), x)[1], 0)

    def result_copy(index):
        return pltpu.make_async_remote_copy(
            src_ref=pbuf.at[index],
            dst_ref=retbuf.at[h, home_slot],
            send_sem=ret_send.at[index],
            recv_sem=ret_recv.at[h, home_slot],
            device_id={"seq": index // C, "sub": index % C, "heads": home},
            device_id_type=MESH,
        )

    def multiply(zb):
        summed = jnp.zeros((C * rows, cols), jnp.float32)
        for g in range(G):
            from_partner(attbuf, at_send, at_recv, zb, g)
            summed = summed + jnp.dot(
                attbuf[pl.ds(zb * C, C), g].reshape(C * rows, width),
                proj[g * width:(g + 1) * width, :],
                preferred_element_type=jnp.float32,
            )
        summed = summed.astype(jnp.bfloat16)
        for k in range(C):
            index = zb * C + k
            pbuf[index] = summed[k * rows:(k + 1) * rows]
            here = (index == own) & (home == h)

            @pl.when(here)
            def _():
                retbuf[h, home_slot] = summed[k * rows:(k + 1) * rows]

            @pl.when(jnp.logical_not(here))
            def _():
                result_copy(index).start()

    launch(kvbuf, kv_send, kv_recv, 0)
    kv_relay(jnp.int32(0))
    q_copy.wait()

    def head_step(g, carry):
        attention(g)
        launch(attbuf, at_send, at_recv, g)
        return carry

    lax.fori_loop(0, G, head_step, 0)
    proj_copy.wait()
    multiply(z)

    def step(d, carry):
        lax.fori_loop(0, G, lambda g, x: (relay(attbuf, at_send, at_recv, d, g), x)[1], 0)

        @pl.when(z - d >= 0)
        def _():
            multiply(z - d)

        @pl.when(z + d < S)
        def _():
            multiply(z + d)

        return carry

    lax.fori_loop(1, S, step, 0)

    res_copy.wait()
    squares = jnp.zeros((rows, 1), jnp.float32)
    for b in range(blocks):
        where = slice(b * cols, (b + 1) * cols)
        value = res_ref[:, where].astype(jnp.float32)
        for k in range(H):
            @pl.when(jnp.logical_not((home == h) & (home_slot == b) & (k == h)))
            def _():
                pltpu.make_async_remote_copy(
                    src_ref=pbuf.at[0], dst_ref=retbuf.at[k, b],
                    send_sem=ret_send.at[0], recv_sem=ret_recv.at[k, b],
                    device_id={"heads": home}, device_id_type=MESH,
                ).wait_recv()
            value = value + retbuf[k, b].astype(jnp.float32)
        hidden = value.astype(jnp.bfloat16)
        hidden_out[:, where] = hidden
        wide = hidden.astype(jnp.float32)
        squares = squares + jnp.sum(wide * wide, axis=-1, keepdims=True)

    ebuf[h] = jnp.broadcast_to(squares, (rows, 128))

    def share(k, side):
        other = (h + k) % H if side == 0 else (h + H - k) % H
        return pltpu.make_async_remote_copy(
            src_ref=ebuf.at[h], dst_ref=ebuf.at[h if side == 0 else other],
            send_sem=en_send.at[k], recv_sem=en_recv.at[h if side == 0 else other],
            device_id={"heads": (h + k) % H}, device_id_type=MESH,
        )

    for k in range(1, H):
        share(k, 0).start()
    for k in range(1, H):
        share(k, 1).wait_recv()
    energy = ebuf[0]
    for k in range(1, H):
        energy = energy + ebuf[k]
    inverse = lax.rsqrt(energy[:, 0:1] / (H * res_ref.shape[1]) + 1e-06)
    for b in range(blocks):
        where = slice(b * cols, (b + 1) * cols)
        normed_out[:, where] = (
            hidden_out[:, where].astype(jnp.float32) * inverse * gain_ref[:, where]
        ).astype(jnp.bfloat16)

    for k in range(1, H):
        share(k, 0).wait_send()

    def finish(i, carry):
        zs, g = i // G, i % G
        drain(kvbuf, kv_send, kv_recv, zs, g)
        drain(attbuf, at_send, at_recv, zs, g)
        return carry

    lax.fori_loop(0, S * G, finish, 0)

    def finish_results(index, carry):
        @pl.when(jnp.logical_not((index == own) & (home == h)))
        def _():
            result_copy(index).wait_send()
        return carry

    lax.fori_loop(0, n, finish_results, 0)


def shards(dims, queries, keys, values, half_order, frame_lengths, out_proj, residual_in, norm_gain):
    S, C, H = dims
    n = S * C
    rows = queries.shape[0]
    G = keys.shape[1] // HEAD_WIDTH
    width = queries.shape[1] // G
    cols = out_proj.shape[1]
    hbm = pl.BlockSpec(memory_space=pltpu.HBM)
    vmem = pl.BlockSpec(memory_space=pltpu.VMEM)
    smem = pl.BlockSpec(memory_space=pltpu.SMEM)
    dma = pltpu.SemaphoreType.DMA
    bf16, f32 = jnp.bfloat16, jnp.float32
    return pl.pallas_call(
        functools.partial(kernel, (S, C, H, G)),
        out_shape=(
            jax.ShapeDtypeStruct(queries.shape, bf16),
            jax.ShapeDtypeStruct(residual_in.shape, bf16),
            jax.ShapeDtypeStruct(residual_in.shape, bf16),
        ),
        in_specs=[smem, smem, hbm, vmem, vmem, hbm, hbm, vmem],
        out_specs=(vmem, vmem, vmem),
        scratch_shapes=[
            pltpu.VMEM((n, G, 2, rows, HEAD_WIDTH), bf16),
            pltpu.VMEM((n, G, rows, width), bf16),
            pltpu.VMEM(out_proj.shape, bf16),
            pltpu.VMEM(queries.shape, bf16),
            pltpu.VMEM(residual_in.shape, bf16),
            pltpu.VMEM((rows, n * rows), f32),
            pltpu.VMEM((n, rows, cols), bf16),
            pltpu.VMEM((H, n // H, rows, cols), bf16),
            pltpu.VMEM((H, rows, 128), f32),
            dma((3,)),
            dma((3, S, G)),
            dma((n, G)),
            dma((3, S, G)),
            dma((n, G)),
            dma((n,)),
            dma((H, n // H)),
            dma((H,)),
            dma((H,)),
        ],
        compiler_params=pltpu.CompilerParams(
            collective_id=0, has_side_effects=True, vmem_limit_bytes=51 * 1024 * 1024
        ),
    )(half_order, frame_lengths, queries, keys, values, out_proj, residual_in, norm_gain[None, :])


def solution(mesh):
    dims = (mesh.shape["seq"], mesh.shape["sub"], mesh.shape["heads"])
    token = P(("groups", "seq", "sub"), "heads")
    in_specs = (
        token, token, token, P("groups"), P("groups"),
        P("heads", ("seq", "sub")), token, P("heads"),
    )
    return jax.shard_map(
        functools.partial(shards, dims), mesh=mesh, in_specs=in_specs,
        out_specs=(token, token, token), check_vma=False,
    )
```
